32 devices in a mesh: grp: 4 (over x, core), ctx: 8 (over z, y).
Axes of the slice: x: 2, y: 2, z: 4, core: 2. Of those that a mesh axis runs over, the one named last changes fastest.
Arguments:
- queries: bfloat16 [4096, 4096], P(('grp', 'ctx')), parts along dimension 0, may hold values from -8 to 8
- key_states: bfloat16 [4096, 512], P(('grp', 'ctx')), parts along dimension 0, may hold values from -8 to 8
- value_states: bfloat16 [4096, 512], P(('grp', 'ctx')), parts along dimension 0, may hold values from -6 to 6
- grads_out: bfloat16 [4096, 4096], P(('grp', 'ctx')), parts along dimension 0, may hold values from -6 to 6
- doc_lengths: int32 [32], P('grp'), parts along dimension 0, may hold values from 1 to 256, as said below
- block_plan: int32 [64], P('grp'), parts along dimension 0, may hold values from 0 to 15, as said below
- needed: int32 [32, 2], P('grp'), parts along dimension 0, may hold values from 0 to 15, as said below
Outputs:
- outputs: bfloat16 [4096, 4096], P(('grp', 'ctx')), parts along dimension 0
- query_grads: bfloat16 [4096, 4096], P(('grp', 'ctx')), parts along dimension 0
- key_grads: bfloat16 [4096, 512], P(('grp', 'ctx')), parts along dimension 0
- value_grads: bfloat16 [4096, 512], P(('grp', 'ctx')), parts along dimension 0
The draws below stay inside these ranges and needn't reach their ends.
There are 4 independent parts, one for each index of `grp`. The reference program is written for one: setup_inputs(seed, part) draws one part's arguments, and reference() takes and returns one part's arrays. A program takes and returns all parts, laid end to end along the dimension named above; each array names one. Nothing has to cross between parts.
Inputs may be any that keep to these rules, and one draw needn't show every extreme that they name: `doc_lengths`: the lengths sum to 1024 and one of them is exactly 256. `block_plan`: each block position appears once. `needed`: each row lists 2 different stored block numbers, no two of which have the same value of block number // 2.
All inputs are finite; a program needn't handle non-finite values.
Results may differ from the reference program's by a relative error of at most 0.013.
Values may be sent and summed in bfloat16 or wider, within the bound.
A program may use at most 128 MiB of HBM per device.

```python
import math
import jax
import jax.numpy as jnp
from jax import lax

HEADS = 32
KV_HEADS = 4
HEAD_DIM = 128
BLK = 64
NDOC = 8
TOK_DEV = 128
NBLK = 16
TOKENS = 1024
NEED = 2
N_CTX = 8


def plan_parts(key):
    base = jax.random.fold_in(key, 7001)
    big_key, weight_key, plan_key, rank_key = jax.random.split(base, 4)
    doc_slots = jnp.arange(NDOC, dtype=jnp.int32)
    big_doc = jax.random.randint(big_key, (), 0, NDOC, dtype=jnp.int32)
    weights = jnp.where(doc_slots == big_doc, 0, jax.random.randint(weight_key, (NDOC,), 2, 5, dtype=jnp.int32))
    remaining = TOKENS - TOKENS // 4
    shares = remaining * weights // jnp.sum(weights)
    shares = shares + jnp.where(doc_slots == (big_doc + 1) % NDOC, remaining - jnp.sum(shares), 0)
    lengths = jnp.where(doc_slots == big_doc, TOKENS // 4, shares).astype(jnp.int32)
    plan = jax.random.permutation(plan_key, NBLK).astype(jnp.int32)
    return (lengths, plan, rank_key)


def draw_queries(key, part):
    normal_key = jax.random.fold_in(jax.random.fold_in(key, 11), 0)
    sampled = jnp.clip(jax.random.normal(normal_key, (TOKENS, HEADS * HEAD_DIM), jnp.float32), -6.0, 6.0)
    return sampled.astype(jnp.bfloat16)


def draw_key_states(key, part):
    sampled = jnp.clip(jax.random.normal(jax.random.fold_in(key, 13), (TOKENS, KV_HEADS * HEAD_DIM), jnp.float32), -6.0, 6.0)
    return sampled.astype(jnp.bfloat16)


def draw_doc_lengths(key, part):
    lengths, plan, rank_key = plan_parts(key)
    return lengths


def draw_block_plan(key, part):
    lengths, plan, rank_key = plan_parts(key)
    return plan


def draw_needed(key, part):
    lengths, plan, rank_key = plan_parts(key)
    ends = jnp.cumsum(lengths).astype(jnp.int32)

    def doc_of(points):
        return jnp.sum((ends[None, :] <= points[:, None]).astype(jnp.int32), axis=1)
    first_doc = doc_of(plan * BLK)
    last_doc = doc_of(plan * BLK + BLK - 1)
    owners = NBLK // 2
    owner_ids = jnp.arange(owners, dtype=jnp.int32)
    query_blocks = jnp.stack([2 * owner_ids, 2 * owner_ids + 1], axis=1)
    query_plan = jnp.take(plan, query_blocks)
    query_first = jnp.take(first_doc, query_blocks)
    useful = (plan[None, None, :] < query_plan[:, :, None]) & (last_doc[None, None, :] == query_first[:, :, None])
    useful = jnp.any(useful, axis=1)
    ranks = jax.vmap(lambda row_key: jax.random.permutation(row_key, NBLK))(jax.random.split(rank_key, owners))
    score = useful.astype(jnp.int32) * NBLK + ranks.astype(jnp.int32)
    paired = score.reshape(owners, owners, 2)
    second = (paired[:, :, 1] > paired[:, :, 0]).astype(jnp.int32)
    owner_score = jnp.max(paired, axis=2)
    owner_block = 2 * owner_ids[None, :] + second
    order = jnp.argsort(-owner_score, axis=1, stable=True)[:, :NEED]
    return jnp.take_along_axis(owner_block, order, axis=1).astype(jnp.int32)


def steps_of(rng, shape, shards, low, top_value):
    gain = 1.0
    for position, shards_of in shards:
        steps = jax.random.uniform(jax.random.fold_in(jax.random.fold_in(rng, 6), position), (shards_of,), jnp.float32, low / len(shards), top_value / len(shards))
        gain = gain * jnp.repeat(jnp.exp(steps), shape[position] // shards_of).reshape((-1,) + (1,) * (len(shape) - 1 - position))
    return gain


def noise(key, extent, scale, bound, cuts=(), held_as=jnp.bfloat16):
    values = scale * jax.random.normal(key, extent, jnp.float32)
    if cuts:
        values = values * steps_of(key, extent, cuts, -0.22, 0.18)
    return jnp.clip(values, -bound, bound).astype(held_as)


def setup_inputs(seed: int = 0, part: int = 0) -> dict:
    key_list = jax.random.split(jax.random.key(seed), 8)
    part_splits = jax.random.split(jax.random.fold_in(key_list[7], part), 8)
    queries = draw_queries(jax.random.fold_in(jax.random.fold_in(key_list[7], part), 71), part)
    key_states = draw_key_states(jax.random.fold_in(jax.random.fold_in(key_list[7], part), 71), part)
    value_states = noise(part_splits[2], (TOKENS, KV_HEADS * HEAD_DIM), 1.0, 6.0, ((0, 8),))
    grads_out = noise(part_splits[3], (TOKENS, HEADS * HEAD_DIM), 1.0, 6.0, ((0, 8),))
    doc_lengths = draw_doc_lengths(jax.random.fold_in(jax.random.fold_in(key_list[7], part), 71), part)
    block_plan = draw_block_plan(jax.random.fold_in(jax.random.fold_in(key_list[7], part), 71), part)
    needed = draw_needed(jax.random.fold_in(jax.random.fold_in(key_list[7], part), 71), part)
    return dict(queries=queries, key_states=key_states, value_states=value_states, grads_out=grads_out, doc_lengths=doc_lengths, block_plan=block_plan, needed=needed)


masked_score = -1e+30

def token_labels(block_plan, doc_ends):
    stored = jnp.arange(TOKENS, dtype=jnp.int32)
    stored_block = stored // BLK
    placed = jnp.take(block_plan, stored_block).astype(jnp.int32) * BLK + stored % BLK
    documents = lax.optimization_barrier(jnp.sum((doc_ends[None, :] <= placed[:, None]).astype(jnp.int32), axis=1))
    return (stored_block, placed, documents)

def reference(queries, key_states, value_states, grads_out, doc_lengths, block_plan, needed):
    score_scale = 1.0 / math.sqrt(HEAD_DIM)
    group_heads = HEADS // KV_HEADS
    doc_ends = jnp.cumsum(doc_lengths).astype(jnp.int32)
    key_block, key_place, key_doc = token_labels(block_plan, doc_ends)
    keys_grouped = key_states.astype(jnp.float32).reshape(TOKENS, KV_HEADS, HEAD_DIM)
    values_grouped = value_states.astype(jnp.float32).reshape(TOKENS, KV_HEADS, HEAD_DIM)

    def per_rank(carried, inputs):
        key_sum, value_sum = carried
        rank_queries, rank_grads, wanted, own_rank = inputs
        first_row = own_rank * TOK_DEV
        query_block = lax.dynamic_slice_in_dim(key_block, first_row, TOK_DEV)
        query_place = lax.dynamic_slice_in_dim(key_place, first_row, TOK_DEV)
        query_doc = lax.dynamic_slice_in_dim(key_doc, first_row, TOK_DEV)
        listed = jnp.any(wanted[:, None] == key_block[None, :], axis=0)
        allowed = listed[None, :] | (query_block[:, None] == key_block[None, :])
        visible_pairs = allowed & (query_doc[:, None] == key_doc[None, :]) & (key_place[None, :] <= query_place[:, None])
        grouped = rank_queries.astype(jnp.float32).reshape(TOK_DEV, KV_HEADS, group_heads, HEAD_DIM)
        scores = jnp.einsum('qhgd,khd->hgqk', grouped, keys_grouped) * score_scale
        scores = jnp.where(visible_pairs, scores, masked_score)
        highest = lax.optimization_barrier(jnp.max(scores, axis=-1))
        totals = lax.optimization_barrier(jnp.sum(jnp.where(visible_pairs, jnp.exp(scores - highest[..., None]), 0.0), axis=-1))
        log_total = highest + jnp.log(totals)
        soft_weights = jnp.where(visible_pairs, jnp.exp(scores - log_total[..., None]), 0.0)
        probs_low = lax.optimization_barrier(soft_weights.astype(jnp.bfloat16)).astype(jnp.float32)
        attended = jnp.einsum('hgqk,khd->qhgd', soft_weights, values_grouped)
        outputs = attended.reshape(TOK_DEV, HEADS * HEAD_DIM).astype(jnp.bfloat16)
        gradient_rows = rank_grads.astype(jnp.float32).reshape(TOK_DEV, KV_HEADS, group_heads, HEAD_DIM)
        products = gradient_rows * outputs.astype(jnp.float32).reshape(TOK_DEV, KV_HEADS, group_heads, HEAD_DIM)
        row_delta = jnp.transpose(lax.optimization_barrier(jnp.sum(products, axis=-1)), (1, 2, 0))
        prob_grads = jnp.einsum('qhgd,khd->hgqk', gradient_rows, values_grouped)
        score_grads = (soft_weights * (prob_grads - row_delta[..., None])).astype(jnp.bfloat16)
        score_grads = lax.optimization_barrier(score_grads).astype(jnp.float32)
        query_part = jnp.einsum('hgqk,khd->qhgd', score_grads, keys_grouped) * score_scale
        query_grads = query_part.reshape(TOK_DEV, HEADS * HEAD_DIM).astype(jnp.bfloat16)
        key_part = jnp.einsum('hgqk,qhgd->khd', score_grads, grouped) * score_scale
        value_part = jnp.einsum('hgqk,qhgd->khd', probs_low, gradient_rows)
        key_low = lax.optimization_barrier(key_part.reshape(TOKENS, -1).astype(jnp.bfloat16))
        value_low = lax.optimization_barrier(value_part.reshape(TOKENS, -1).astype(jnp.bfloat16))
        key_sum = key_sum + key_low.astype(jnp.float32)
        value_sum = value_sum + value_low.astype(jnp.float32)
        return ((key_sum, value_sum), (outputs, query_grads))
    empty_sum = jnp.zeros((TOKENS, KV_HEADS * HEAD_DIM), jnp.float32)
    inputs = (queries.reshape(N_CTX, TOK_DEV, HEADS * HEAD_DIM), grads_out.reshape(N_CTX, TOK_DEV, HEADS * HEAD_DIM), needed, jnp.arange(N_CTX, dtype=jnp.int32))
    sums, stacked = lax.scan(per_rank, (empty_sum, empty_sum), inputs)
    outputs = stacked[0].reshape(TOKENS, HEADS * HEAD_DIM)
    query_grads = stacked[1].reshape(TOKENS, HEADS * HEAD_DIM)
    return (outputs, query_grads, sums[0].astype(jnp.bfloat16), sums[1].astype(jnp.bfloat16))
```

```python
import functools
import math

import jax
import jax.numpy as jnp
from jax import lax
from jax.experimental import pallas as pl
from jax.experimental.pallas import tpu as pltpu
from jax.sharding import PartitionSpec as P

HEADS = 32
KV_HEADS = 4
HEAD_DIM = 128
BLK = 64
GROUP = HEADS // KV_HEADS
PIECES = 2 * KV_HEADS
PAIR = 2

masked_score = -1e30


def lane_count(n):
    lanes = 1
    for y in range(1, n + 1):
        if n % (2 * y) == 0 and 2 * y * y <= n:
            lanes = y
    return lanes


def matmul(a, b, contract):
    return lax.dot_general(
        a, b, ((contract[:1], contract[1:]), ((), ())), preferred_element_type=jnp.float32
    )


def kernel(n, q_hbm, k_hbm, v_hbm, do_hbm, doc_hbm, plan_hbm, need_hbm, *rest):
    out_ref, dq_ref, dk_ref, dv_ref = rest[:4]
    q_buf, do_buf, key_acc, value_acc, bias, doc_ref, plan_ref, need_ref = rest[4:12]
    rest = rest[12:]
    col, zs, zr, gz, ys, yr, ms, mr = (rest[i * PIECES : (i + 1) * PIECES] for i in range(8))
    (
        wide_sem,
        own_sem,
        table_sem,
        m_send,
        m_recv,
        yo_send,
        yo_recv,
        yr_send,
        yr_recv,
        z_send,
        z_recv,
        bz_send,
        bz_recv,
        by_send,
        by_recv,
        bm_send,
        bm_recv,
    ) = rest[8 * PIECES :]
    rows = q_buf.shape[0]
    own_blocks = rows // BLK
    listed_count = need_ref.shape[0]
    lanes = lane_count(n)
    columns = n // lanes
    half = columns // 2
    me = lax.axis_index("ctx")
    lane, column = lax.rem(me, lanes), me // lanes
    left = column < half
    place = jnp.where(left, column, columns - 1 - column)
    score_scale = 1.0 / math.sqrt(HEAD_DIM)
    chunk_cols = GROUP * HEAD_DIM

    def at_place(p, y):
        return jnp.where(left, p, columns - 1 - p) * lanes + y

    mirror = (columns - 1 - column) * lanes + lane
    lane_peer = [column * lanes + lax.rem(lane + o, lanes) for o in range(lanes)]
    place_peer = [at_place(lax.rem(place + o, half), lane) for o in range(half)]
    place_source = [at_place(lax.rem(place + half - o, half), lane) for o in range(half)]

    barrier = pltpu.get_barrier_semaphore()
    friends = [mirror] + lane_peer[1:] + place_peer[1:]
    for peer in friends:
        pl.semaphore_signal(
            barrier, inc=1, device_id={"ctx": peer}, device_id_type=pl.DeviceIdType.MESH
        )

    own_at = pl.ds(lane * 2 * own_blocks, own_blocks)
    relayed_at = pl.ds((lane * 2 + 1) * own_blocks, own_blocks)
    own_loads, loads = [], {}
    for p in range(PIECES):
        src = (k_hbm, v_hbm)[p % 2].at[:, :, pl.ds(p // 2 * HEAD_DIM, HEAD_DIM)]
        own_loads.append(pltpu.make_async_copy(src, col[p].at[own_at], own_sem.at[p]))
        own_loads[p].start()
    tables = [
        pltpu.make_async_copy(src, dst, table_sem.at[i])
        for i, (src, dst) in enumerate(
            ((doc_hbm, doc_ref), (plan_hbm, plan_ref), (need_hbm, need_ref))
        )
    ]
    for t in tables:
        t.start()
    for c in range(KV_HEADS):
        cols = pl.ds(c * chunk_cols, chunk_cols)
        for i, (src, dst) in enumerate(((q_hbm, q_buf), (do_hbm, do_buf))):
            loads[i, c] = pltpu.make_async_copy(
                src.at[:, cols], dst.at[:, cols], wide_sem.at[i, c]
            )
            loads[i, c].start()

    started = []

    def send(src, dst, sems, at, peer):
        copy = pltpu.make_async_remote_copy(
            src_ref=src,
            dst_ref=dst,
            send_sem=sems[0].at[at],
            recv_sem=sems[1].at[at],
            device_id={"ctx": peer},
            device_id_type=pl.DeviceIdType.MESH,
        )
        copy.start()
        started.append(copy)
        return copy

    for p in range(PIECES):
        own_loads[p].wait()
    pl.semaphore_wait(barrier, len(friends))
    to_mirror, to_lane, relays, to_place = [], [], {}, {}
    for p in range(PIECES):
        own = col[p].at[own_at]
        to_mirror.append(send(own, col[p].at[relayed_at], (m_send, m_recv), (p,), mirror))
    for p in range(PIECES):
        own = col[p].at[own_at]
        to_lane.append(
            [send(own, own, (yo_send, yo_recv), (p, o - 1), lane_peer[o]) for o in range(1, lanes)]
        )

    for t in tables:
        t.wait()
    ends, total = [], jnp.int32(0)
    for d in range(doc_ref.shape[0]):
        total = total + doc_ref[d]
        ends.append(total)

    def documents(at):
        doc = jnp.zeros_like(at)
        for end in ends:
            doc = doc + (at >= end).astype(jnp.int32)
        return doc

    key_row = lax.broadcasted_iota(jnp.int32, (BLK, rows), 0)
    query_col = lax.broadcasted_iota(jnp.int32, (BLK, rows), 1)
    query_local = query_col // BLK
    query_place = query_col
    for b in range(own_blocks):
        shift = (plan_ref[me * own_blocks + b] - b) * BLK
        query_place = jnp.where(query_local == b, query_col + shift, query_place)
    query_doc = documents(query_place)
    listed = [need_ref[j, me] for j in range(listed_count)]
    for s in range(own_blocks + listed_count):
        if s < own_blocks:
            block = me * own_blocks + s
            found = jnp.int32(0)
            for b in listed:
                found = jnp.where(b == block, 1, found)
            allowed = jnp.where(query_local == s, 1, found)
        else:
            block = listed[s - own_blocks]
            allowed = jnp.where(block // own_blocks == me, 0, jnp.ones_like(query_col))
        key_place = key_row + plan_ref[block] * BLK
        visible = (allowed > 0) & (documents(key_place) == query_doc) & (key_place <= query_place)
        bias[s * BLK : (s + 1) * BLK, :] = jnp.where(visible, 0.0, masked_score)

    def in_column(block):
        owner = block // own_blocks
        owner_left = owner // lanes < half
        side = jnp.where(owner_left == left, 0, 1)
        return ((owner % lanes) * 2 + side) * own_blocks + block % own_blocks

    def place_of(block):
        at = block // own_blocks // lanes
        return jnp.minimum(at, columns - 1 - at)

    chosen = [
        [in_column(need_ref[j, place_peer[o]]) for j in range(listed_count)] for o in range(half)
    ]
    slots = [lax.rem(place - place_of(b) + half, half) for b in listed]

    def relay(c):
        for p in (2 * c, 2 * c + 1):
            to_mirror[p].wait_recv()
            mine = col[p].at[relayed_at]
            relays[p] = [
                send(mine, mine, (yr_send, yr_recv), (p, o - 1), lane_peer[o])
                for o in range(1, lanes)
            ]

    def choose(c):
        for p in (2 * c, 2 * c + 1):
            for copy in to_lane[p] + relays[p]:
                copy.wait_recv()
            for o in list(range(1, half)) + [0]:
                for j in range(listed_count):
                    value = col[p][chosen[o][j]]
                    if o:
                        zs[p][o - 1, j] = value
                    else:
                        zr[p][0, j] = value
                if o:
                    to_place[p, o] = send(
                        zs[p].at[o - 1], zr[p].at[o], (z_send, z_recv), (p, o - 1), place_peer[o]
                    )

    exponent = score_scale * math.log2(math.e)
    state = {}

    def begin(c):
        loads[0, c].wait()
        loads[1, c].wait()
        whole = []
        for p in (2 * c, 2 * c + 1):
            for o in range(1, half):
                to_place[p, o].wait_recv()
            pieces = [col[p][lane * 2 * own_blocks + b] for b in range(own_blocks)]
            pieces += [zr[p][slots[j], j] for j in range(listed_count)]
            whole.append(jnp.concatenate(pieces, axis=0))
        keys, values = whole
        state[c] = dict(keys=keys, values=values, keys_t=keys.T, values_t=values.T)

    def attend(c, pair):
        s = state[c]
        heads = [
            slice(
                (c * GROUP + pair * PAIR + x) * HEAD_DIM,
                (c * GROUP + pair * PAIR + x + 1) * HEAD_DIM,
            )
            for x in range(PAIR)
        ]
        queries = jnp.concatenate([q_buf[:, at] for at in heads], axis=0)
        grads = jnp.concatenate([do_buf[:, at] for at in heads], axis=0)
        mask = bias[...]
        scores = matmul(s["keys"], queries, (1, 1)) + jnp.concatenate([mask] * PAIR, axis=1)
        highest = jnp.max(scores, axis=0, keepdims=True)
        weights = jnp.exp2((scores - highest) * exponent)
        weights = weights * (1.0 / jnp.sum(weights, axis=0, keepdims=True))
        low = weights.astype(jnp.bfloat16)
        attended = matmul(s["values_t"], low, (1, 0)).T.astype(jnp.bfloat16)
        prob_grads = matmul(s["values"], grads, (1, 1))
        delta = jnp.sum(weights * prob_grads, axis=0, keepdims=True)
        score_grads = (weights * (prob_grads - delta)).astype(jnp.bfloat16)
        query_grad = (matmul(s["keys_t"], score_grads, (1, 0)) * score_scale).T
        query_grad = query_grad.astype(jnp.bfloat16)
        for x, at in enumerate(heads):
            out_ref[:, at] = attended[x * rows : (x + 1) * rows]
            dq_ref[:, at] = query_grad[x * rows : (x + 1) * rows]
        more_keys = matmul(score_grads, queries, (1, 0))
        more_values = matmul(low, grads, (1, 0))
        if pair == 0:
            s["key_grad"], s["value_grad"] = more_keys, more_values
        else:
            s["key_grad"] = s["key_grad"] + more_keys
            s["value_grad"] = s["value_grad"] + more_values

    back_place, back_lane, back_mirror = {}, {}, {}

    def finish(c):
        s = state.pop(c)
        at = slice(c * HEAD_DIM, (c + 1) * HEAD_DIM)
        for p, acc, grad in (
            (2 * c + 1, value_acc, s["value_grad"]),
            (2 * c, key_acc, s["key_grad"] * score_scale),
        ):
            for j in range(listed_count):
                first = rows + j * BLK
                gz[p][0, j] = grad[first : first + BLK].astype(jnp.bfloat16)
            for o in range(1, half):
                back_place[p, o] = send(
                    gz[p].at[0], gz[p].at[o], (bz_send, bz_recv), (p, o - 1), place_peer[o]
                )
            acc[:, at] = grad[:rows]

    def block_of(side, y, b):
        at = column if side == 0 else columns - 1 - column
        return (at * lanes + y) * own_blocks + b

    def collect(p, side, y):
        targets = [block_of(side, y, b) for b in range(own_blocks)]
        zero = jnp.zeros((BLK, HEAD_DIM), jnp.float32)
        if half * listed_count <= 8:
            sums = [zero] * own_blocks
            for o in range(half):
                for j in range(listed_count):
                    block = need_ref[j, place_source[o]]
                    part = gz[p][o, j].astype(jnp.float32)
                    sums = [
                        x + jnp.where(block == t, part, 0.0)
                        for x, t in zip(sums, targets, strict=True)
                    ]
            return sums

        def add(i, sums):
            o, j = i // listed_count, i % listed_count
            block = need_ref[j, at_place(lax.rem(place + half - o, half), lane)]
            part = gz[p][o, j].astype(jnp.float32)
            return tuple(
                x + jnp.where(block == t, part, 0.0) for x, t in zip(sums, targets, strict=True)
            )

        return list(lax.fori_loop(0, half * listed_count, add, (zero,) * own_blocks))

    def spread(c):
        for p in (2 * c + 1, 2 * c):
            for o in range(1, half):
                back_place[p, o].wait_recv()
            for side in (1, 0):
                for o in range(1, lanes):
                    for b, x in enumerate(collect(p, side, lax.rem(lane + o, lanes))):
                        ys[p][o - 1, side, b] = x.astype(jnp.bfloat16)
                    back_lane[p, side, o] = send(
                        ys[p].at[o - 1, side],
                        yr[p].at[o - 1, side],
                        (by_send, by_recv),
                        (p, side, o - 1),
                        lane_peer[o],
                    )

    def reflect(c):
        for p in (2 * c + 1, 2 * c):
            for o in range(1, lanes):
                back_lane[p, 1, o].wait_recv()
            for b, x in enumerate(collect(p, 1, lane)):
                for o in range(1, lanes):
                    x = x + yr[p][o - 1, 1, b].astype(jnp.float32)
                ms[p][b] = x.astype(jnp.bfloat16)
            back_mirror[p] = send(ms[p], mr[p], (bm_send, bm_recv), (p,), mirror)

    def settle(c):
        at = slice(c * HEAD_DIM, (c + 1) * HEAD_DIM)
        for p, acc, result in ((2 * c + 1, value_acc, dv_ref), (2 * c, key_acc, dk_ref)):
            for o in range(1, lanes):
                back_lane[p, 0, o].wait_recv()
            sums = collect(p, 0, lane)
            back_mirror[p].wait_recv()
            for b, x in enumerate(sums):
                for o in range(1, lanes):
                    x = x + yr[p][o - 1, 0, b].astype(jnp.float32)
                x = x + mr[p][b].astype(jnp.float32) + acc[b * BLK : (b + 1) * BLK, at]
                result[b * BLK : (b + 1) * BLK, at] = x.astype(jnp.bfloat16)

    pairs = GROUP // PAIR
    last = KV_HEADS - 1
    relay(0)
    relay(1)
    choose(0)
    for c in range(2, last):
        relay(c)
        choose(c - 1)
    for c in range(KV_HEADS):
        begin(c)
        for pair in range(pairs):
            if pair == pairs // 2:
                if c == 0:
                    relay(last)
                if c == 1:
                    choose(last)
            attend(c, pair)
        finish(c)
        if c == 0:
            choose(last - 1)
        if c >= 1:
            spread(c - 1)
        if c >= 2:
            reflect(c - 2)
    settle(0)
    spread(last)
    reflect(last - 1)
    settle(1)
    reflect(last)
    for c in range(2, KV_HEADS):
        settle(c)
    for copy in started:
        copy.wait_send()


def write_out(*refs):
    sources, results, sem = refs[:4], refs[4:8], refs[8]
    copies = [
        pltpu.make_async_copy(src, dst, sem.at[i])
        for i, (src, dst) in enumerate(zip(sources, results, strict=True))
    ]
    for copy in copies:
        copy.start()
    for copy in copies:
        copy.wait()


def on_device(queries, key_states, value_states, grads_out, doc_lengths, block_plan, needed):
    n = lax.axis_size("ctx")
    rows, width = queries.shape
    kv_width = key_states.shape[1]
    own_blocks = rows // BLK
    blocked = (own_blocks, BLK, kv_width)
    listed = needed.shape[1]
    lanes = lane_count(n)
    half = n // lanes // 2
    vmem = pl.BlockSpec(memory_space=pltpu.VMEM)
    hbm = pl.BlockSpec(memory_space=pltpu.HBM)
    anywhere = pl.BlockSpec(memory_space=pl.ANY)
    wide = jax.ShapeDtypeStruct((rows, width), jnp.bfloat16)
    narrow = jax.ShapeDtypeStruct((rows, kv_width), jnp.bfloat16)
    results = (wide, wide, narrow, narrow)

    def store(*lead):
        return [pltpu.VMEM((*lead, BLK, HEAD_DIM), jnp.bfloat16)] * PIECES

    def sems(*shape):
        return [pltpu.SemaphoreType.DMA((PIECES, *shape))] * 2

    peers, others = max(lanes - 1, 1), max(half - 1, 1)
    parts = pl.pallas_call(
        functools.partial(kernel, n),
        out_shape=results,
        in_specs=[hbm] * 7,
        out_specs=(vmem,) * 4,
        scratch_shapes=[pltpu.VMEM((rows, width), jnp.bfloat16)] * 2
        + [pltpu.VMEM((rows, kv_width), jnp.float32)] * 2
        + [pltpu.VMEM((rows + listed * BLK, rows), jnp.float32)]
        + [pltpu.SMEM(x.shape, jnp.int32) for x in (doc_lengths, block_plan, needed.T)]
        + store(lanes * 2 * own_blocks)
        + store(others, listed)
        + store(half, listed)
        + store(half, listed)
        + store(peers, 2, own_blocks)
        + store(peers, 2, own_blocks)
        + store(own_blocks)
        + store(own_blocks)
        + [pltpu.SemaphoreType.DMA((2, KV_HEADS))]
        + [pltpu.SemaphoreType.DMA((PIECES,))]
        + [pltpu.SemaphoreType.DMA((3,))]
        + sems()
        + sems(peers)
        + sems(peers)
        + sems(others)
        + sems(others)
        + sems(2, peers)
        + sems(),
        compiler_params=pltpu.CompilerParams(
            collective_id=0, has_side_effects=True, vmem_limit_bytes=32 * 1024 * 1024
        ),
    )(
        *(
            pltpu.with_memory_space_constraint(x, pltpu.HBM)
            for x in (
                queries,
                key_states.reshape(blocked),
                value_states.reshape(blocked),
                grads_out,
                doc_lengths,
                block_plan,
                needed.T,
            )
        )
    )
    return pl.pallas_call(
        write_out,
        out_shape=results,
        in_specs=[vmem] * 4,
        out_specs=(anywhere,) * 4,
        scratch_shapes=[pltpu.SemaphoreType.DMA((4,))],
    )(*(pltpu.with_memory_space_constraint(x, pltpu.VMEM) for x in parts))


def solution(mesh):
    tokens = P(("grp", "ctx"), None)
    return jax.shard_map(
        on_device,
        mesh=mesh,
        in_specs=(tokens, tokens, tokens, tokens, P("grp"), P("grp"), P("grp", None)),
        out_specs=(tokens, tokens, tokens, tokens),
        check_vma=False,
    )
```

```python
import functools
import math

import jax
import jax.numpy as jnp
from jax import lax
from jax.experimental import pallas as pl
from jax.experimental.pallas import tpu as pltpu
from jax.sharding import PartitionSpec as P

HEADS = 32
KV_HEADS = 4
HEAD_DIM = 128
BLK = 64
GROUP = HEADS // KV_HEADS
PIECES = 2 * KV_HEADS
PAIR = 2

masked_score = -1e30


def lane_count(n):
    lanes = 1
    for y in range(1, n + 1):
        if n % (2 * y) == 0 and 2 * y * y <= n:
            lanes = y
    return lanes


def matmul(a, b, contract):
    return lax.dot_general(
        a, b, ((contract[:1], contract[1:]), ((), ())), preferred_element_type=jnp.float32
    )


def kernel(n, q_hbm, k_hbm, v_hbm, do_hbm, doc_hbm, plan_hbm, need_hbm, *rest):
    out_ref, dq_ref, dk_ref, dv_ref = rest[:4]
    q_buf, do_buf, key_acc, value_acc, bias, doc_ref, plan_ref, need_ref = rest[4:12]
    own_e, own_dp, own_o, stats, far_s, far_dp, low_buf, ds_buf = rest[12:20]
    rest = rest[20:]
    col, zs, zr, gz, ys, yr, ms, mr = (rest[i * PIECES : (i + 1) * PIECES] for i in range(8))
    (
        wide_sem,
        own_sem,
        table_sem,
        m_send,
        m_recv,
        yo_send,
        yo_recv,
        yr_send,
        yr_recv,
        z_send,
        z_recv,
        bz_send,
        bz_recv,
        by_send,
        by_recv,
        bm_send,
        bm_recv,
    ) = rest[8 * PIECES :]
    rows = q_buf.shape[0]
    own_blocks = rows // BLK
    listed_count = need_ref.shape[0]
    lanes = lane_count(n)
    columns = n // lanes
    half = columns // 2
    me = lax.axis_index("ctx")
    lane, column = lax.rem(me, lanes), me // lanes
    left = column < half
    place = jnp.where(left, column, columns - 1 - column)
    score_scale = 1.0 / math.sqrt(HEAD_DIM)
    chunk_cols = GROUP * HEAD_DIM

    def at_place(p, y):
        return jnp.where(left, p, columns - 1 - p) * lanes + y

    mirror = (columns - 1 - column) * lanes + lane
    lane_peer = [column * lanes + lax.rem(lane + o, lanes) for o in range(lanes)]
    place_peer = [at_place(lax.rem(place + o, half), lane) for o in range(half)]
    place_source = [at_place(lax.rem(place + half - o, half), lane) for o in range(half)]

    barrier = pltpu.get_barrier_semaphore()
    friends = [mirror] + lane_peer[1:] + place_peer[1:]
    for peer in friends:
        pl.semaphore_signal(
            barrier, inc=1, device_id={"ctx": peer}, device_id_type=pl.DeviceIdType.MESH
        )

    own_at = pl.ds(lane * 2 * own_blocks, own_blocks)
    relayed_at = pl.ds((lane * 2 + 1) * own_blocks, own_blocks)
    own_loads, loads = [], {}
    for p in range(PIECES):
        src = (k_hbm, v_hbm)[p % 2].at[:, :, pl.ds(p // 2 * HEAD_DIM, HEAD_DIM)]
        own_loads.append(pltpu.make_async_copy(src, col[p].at[own_at], own_sem.at[p]))
        own_loads[p].start()
    tables = [
        pltpu.make_async_copy(src, dst, table_sem.at[i])
        for i, (src, dst) in enumerate(
            ((doc_hbm, doc_ref), (plan_hbm, plan_ref), (need_hbm, need_ref))
        )
    ]
    for t in tables:
        t.start()
    for c in range(KV_HEADS):
        cols = pl.ds(c * chunk_cols, chunk_cols)
        for i, (src, dst) in enumerate(((q_hbm, q_buf), (do_hbm, do_buf))):
            loads[i, c] = pltpu.make_async_copy(
                src.at[:, cols], dst.at[:, cols], wide_sem.at[i, c]
            )
            loads[i, c].start()

    started = []

    def remote(src, dst, sems, at, peer):
        return pltpu.make_async_remote_copy(
            src_ref=src,
            dst_ref=dst,
            send_sem=sems[0].at[at],
            recv_sem=sems[1].at[at],
            device_id={"ctx": peer},
            device_id_type=pl.DeviceIdType.MESH,
        )

    def send(src, dst, sems, at, peer):
        copy = remote(src, dst, sems, at, peer)
        copy.start()
        started.append(copy)
        return copy

    for p in range(PIECES):
        own_loads[p].wait()
    pl.semaphore_wait(barrier, len(friends))
    to_lane, relays, to_place = [], {}, {}

    to_mirror = [
        remote(col[p].at[own_at], col[p].at[relayed_at], (m_send, m_recv), (p,), mirror)
        for p in range(PIECES)
    ]
    innermost = place == half - 1

    def cross(first, last):
        for p in range(2 * first, 2 * last):
            to_mirror[p].start()

    cross(0, 1)
    pl.when(innermost)(lambda: cross(1, KV_HEADS))
    started += to_mirror

    def release(c):
        pl.when(jnp.logical_not(innermost))(lambda: cross(c, c + 1))
    for p in range(PIECES):
        own = col[p].at[own_at]
        to_lane.append(
            [send(own, own, (yo_send, yo_recv), (p, o - 1), lane_peer[o]) for o in range(1, lanes)]
        )

    for t in tables:
        t.wait()
    ends, total = [], jnp.int32(0)
    for d in range(doc_ref.shape[0]):
        total = total + doc_ref[d]
        ends.append(total)

    def documents(at):
        doc = jnp.zeros_like(at)
        for end in ends:
            doc = doc + (at >= end).astype(jnp.int32)
        return doc

    key_row = lax.broadcasted_iota(jnp.int32, (BLK, rows), 0)
    query_col = lax.broadcasted_iota(jnp.int32, (BLK, rows), 1)
    query_local = query_col // BLK
    query_place = query_col
    for b in range(own_blocks):
        shift = (plan_ref[me * own_blocks + b] - b) * BLK
        query_place = jnp.where(query_local == b, query_col + shift, query_place)
    query_doc = documents(query_place)
    listed = [need_ref[j, me] for j in range(listed_count)]
    for s in range(own_blocks + listed_count):
        if s < own_blocks:
            block = me * own_blocks + s
            found = jnp.int32(0)
            for b in listed:
                found = jnp.where(b == block, 1, found)
            allowed = jnp.where(query_local == s, 1, found)
        else:
            block = listed[s - own_blocks]
            allowed = jnp.where(block // own_blocks == me, 0, jnp.ones_like(query_col))
        key_place = key_row + plan_ref[block] * BLK
        visible = (allowed > 0) & (documents(key_place) == query_doc) & (key_place <= query_place)
        bias[s * BLK : (s + 1) * BLK, :] = jnp.where(visible, 0.0, masked_score)

    def in_column(block):
        owner = block // own_blocks
        owner_left = owner // lanes < half
        side = jnp.where(owner_left == left, 0, 1)
        return ((owner % lanes) * 2 + side) * own_blocks + block % own_blocks

    def place_of(block):
        at = block // own_blocks // lanes
        return jnp.minimum(at, columns - 1 - at)

    chosen = [
        [in_column(need_ref[j, place_peer[o]]) for j in range(listed_count)] for o in range(half)
    ]
    slots = [lax.rem(place - place_of(b) + half, half) for b in listed]

    def relay(c):
        for p in (2 * c, 2 * c + 1):
            to_mirror[p].wait_recv()
            mine = col[p].at[relayed_at]
            relays[p] = [
                send(mine, mine, (yr_send, yr_recv), (p, o - 1), lane_peer[o])
                for o in range(1, lanes)
            ]

    def choose(c):
        for p in (2 * c, 2 * c + 1):
            for copy in to_lane[p] + relays[p]:
                copy.wait_recv()
            for o in list(range(1, half)) + [0]:
                for j in range(listed_count):
                    value = col[p][chosen[o][j]]
                    if o:
                        zs[p][o - 1, j] = value
                    else:
                        zr[p][0, j] = value
                if o:
                    to_place[p, o] = send(
                        zs[p].at[o - 1], zr[p].at[o], (z_send, z_recv), (p, o - 1), place_peer[o]
                    )

    exponent = score_scale * math.log2(math.e)
    span = PAIR * rows
    state = {}

    def heads_of(c, pair):
        first = c * GROUP + pair * PAIR
        return [slice((first + x) * HEAD_DIM, (first + x + 1) * HEAD_DIM) for x in range(PAIR)]

    def stacked(ref, heads):
        return jnp.concatenate([ref[:, at] for at in heads], axis=0)

    def columns_of(c, pair):
        first = (c * GROUP // PAIR + pair) * span
        return slice(first, first + span)

    def own_scores(c, pair):
        heads, at = heads_of(c, pair), columns_of(c, pair)
        mask = jnp.concatenate([bias[:rows]] * PAIR, axis=1)
        own_e[:, at] = matmul(state[c]["own_keys"], stacked(q_buf, heads), (1, 1)) + mask
        own_dp[:, at] = matmul(state[c]["own_values"], stacked(do_buf, heads), (1, 1))

    def own_weights(c, pair):
        at = columns_of(c, pair)
        scores = own_e[:, at]
        highest = jnp.max(scores, axis=0, keepdims=True)
        weights = jnp.exp2((scores - highest) * exponent)
        own_e[:, at] = weights
        stats[0:1, at] = highest
        stats[1:2, at] = jnp.sum(weights, axis=0, keepdims=True)
        stats[2:3, at] = jnp.sum(weights * own_dp[:, at], axis=0, keepdims=True)
        low_buf[pair, :rows] = weights.astype(jnp.bfloat16)

    def own_output(c, pair):
        own_o[:, columns_of(c, pair)] = matmul(
            state[c]["own_values_t"], low_buf[pair, :rows], (1, 0)
        )

    pairs = GROUP // PAIR

    def staged(c, stages):
        for step in range(pairs + len(stages) - 1):
            for i, stage in enumerate(stages):
                if 0 <= step - i < pairs:
                    stage(c, step - i)

    def own_part(c):
        loads[0, c].wait()
        loads[1, c].wait()
        own_keys, own_values = (
            jnp.concatenate([col[p][lane * 2 * own_blocks + b] for b in range(own_blocks)], axis=0)
            for p in (2 * c, 2 * c + 1)
        )
        state[c] = dict(own_keys=own_keys, own_values=own_values, own_values_t=own_values.T)
        staged(c, (own_scores, own_weights, own_output))

    def listed_scores(c, pair):
        heads = heads_of(c, pair)
        mask = jnp.concatenate([bias[rows:]] * PAIR, axis=1)
        far_s[pair] = matmul(state[c]["far_keys"], stacked(q_buf, heads), (1, 1)) + mask
        far_dp[pair] = matmul(state[c]["far_values"], stacked(do_buf, heads), (1, 1))

    def listed_weights(c, pair):
        at = columns_of(c, pair)
        scores, own_highest = far_s[pair], stats[0:1, at]
        highest = jnp.maximum(jnp.max(scores, axis=0, keepdims=True), own_highest)
        weights = jnp.exp2((scores - highest) * exponent)
        own_scale = jnp.exp2((own_highest - highest) * exponent)
        total = jnp.sum(weights, axis=0, keepdims=True) + own_scale * stats[1:2, at]
        inverse = 1.0 / total
        own_scale = own_scale * inverse
        weights = weights * inverse
        prob_grads = far_dp[pair]
        delta = jnp.sum(weights * prob_grads, axis=0, keepdims=True) + own_scale * stats[2:3, at]
        low_buf[pair, rows:] = weights.astype(jnp.bfloat16)
        ds_buf[pair, rows:] = (weights * (prob_grads - delta)).astype(jnp.bfloat16)
        weights = own_e[:, at] * own_scale
        low_buf[pair, :rows] = weights.astype(jnp.bfloat16)
        ds_buf[pair, :rows] = (weights * (own_dp[:, at] - delta)).astype(jnp.bfloat16)
        stats[0:1, at] = own_scale

    def results(c, pair):
        at = columns_of(c, pair)
        attended = matmul(state[c]["far_values_t"], low_buf[pair, rows:], (1, 0))
        attended = attended + own_o[:, at] * stats[0:1, at]
        query_grad = matmul(state[c]["keys_t"], ds_buf[pair], (1, 0)) * score_scale
        for ref, value in ((out_ref, attended), (dq_ref, query_grad)):
            value = value.astype(jnp.bfloat16).T
            for x, head in enumerate(heads_of(c, pair)):
                ref[:, head] = value[x * rows : (x + 1) * rows]

    def begin(c):
        far = []
        for p in (2 * c, 2 * c + 1):
            for o in range(1, half):
                to_place[p, o].wait_recv()
            far.append(
                jnp.concatenate([zr[p][slots[j], j] for j in range(listed_count)], axis=0)
            )
        s = state[c]
        s.update(far_keys=far[0], far_values=far[1], far_values_t=far[1].T)
        s["keys_t"] = jnp.concatenate([s["own_keys"], far[0]], axis=0).T

    def attend(c):
        staged(c, (listed_scores, listed_weights, results))
        s = state[c]
        every = [head for pair in range(pairs) for head in heads_of(c, pair)]
        for name, buf, ref in (("value_grad", low_buf, do_buf), ("key_grad", ds_buf, q_buf)):
            weights = jnp.concatenate([buf[pair] for pair in range(pairs)], axis=1)
            s[name] = matmul(weights, stacked(ref, every), (1, 0))

    back_place, back_lane, back_mirror = {}, {}, {}

    def finish(c):
        s = state.pop(c)
        at = slice(c * HEAD_DIM, (c + 1) * HEAD_DIM)
        for p, acc, grad in (
            (2 * c + 1, value_acc, s["value_grad"]),
            (2 * c, key_acc, s["key_grad"] * score_scale),
        ):
            for j in range(listed_count):
                first = rows + j * BLK
                gz[p][0, j] = grad[first : first + BLK].astype(jnp.bfloat16)
            for o in range(1, half):
                back_place[p, o] = send(
                    gz[p].at[0], gz[p].at[o], (bz_send, bz_recv), (p, o - 1), place_peer[o]
                )
            acc[:, at] = grad[:rows]

    def block_of(side, y, b):
        at = column if side == 0 else columns - 1 - column
        return (at * lanes + y) * own_blocks + b

    def collect(p, side, y):
        targets = [block_of(side, y, b) for b in range(own_blocks)]
        zero = jnp.zeros((BLK, HEAD_DIM), jnp.float32)
        if half * listed_count <= 8:
            sums = [zero] * own_blocks
            for o in range(half):
                for j in range(listed_count):
                    block = need_ref[j, place_source[o]]
                    part = gz[p][o, j].astype(jnp.float32)
                    sums = [
                        x + jnp.where(block == t, part, 0.0)
                        for x, t in zip(sums, targets, strict=True)
                    ]
            return sums

        def add(i, sums):
            o, j = i // listed_count, i % listed_count
            block = need_ref[j, at_place(lax.rem(place + half - o, half), lane)]
            part = gz[p][o, j].astype(jnp.float32)
            return tuple(
                x + jnp.where(block == t, part, 0.0) for x, t in zip(sums, targets, strict=True)
            )

        return list(lax.fori_loop(0, half * listed_count, add, (zero,) * own_blocks))

    def spread(c, side):
        for p in (2 * c + 1, 2 * c):
            if side:
                for o in range(1, half):
                    back_place[p, o].wait_recv()
            for o in range(1, lanes):
                for b, x in enumerate(collect(p, side, lax.rem(lane + o, lanes))):
                    ys[p][o - 1, side, b] = x.astype(jnp.bfloat16)
                back_lane[p, side, o] = send(
                    ys[p].at[o - 1, side],
                    yr[p].at[o - 1, side],
                    (by_send, by_recv),
                    (p, side, o - 1),
                    lane_peer[o],
                )

    def reflect(c):
        for p in (2 * c + 1, 2 * c):
            for o in range(1, lanes):
                back_lane[p, 1, o].wait_recv()
            for b, x in enumerate(collect(p, 1, lane)):
                for o in range(1, lanes):
                    x = x + yr[p][o - 1, 1, b].astype(jnp.float32)
                ms[p][b] = x.astype(jnp.bfloat16)
            back_mirror[p] = send(ms[p], mr[p], (bm_send, bm_recv), (p,), mirror)

    def settle(c):
        at = slice(c * HEAD_DIM, (c + 1) * HEAD_DIM)
        for p, acc, result in ((2 * c + 1, value_acc, dv_ref), (2 * c, key_acc, dk_ref)):
            for o in range(1, lanes):
                back_lane[p, 0, o].wait_recv()
            sums = collect(p, 0, lane)
            back_mirror[p].wait_recv()
            for b, x in enumerate(sums):
                for o in range(1, lanes):
                    x = x + yr[p][o - 1, 0, b].astype(jnp.float32)
                x = x + mr[p][b].astype(jnp.float32) + acc[b * BLK : (b + 1) * BLK, at]
                result[b * BLK : (b + 1) * BLK, at] = x.astype(jnp.bfloat16)

    def compute(c):
        begin(c)
        attend(c)
        finish(c)

    def spread_mirrored(c):
        spread(c, 1)

    def spread_own(c):
        spread(c, 0)

    for stage, chunks in (
        (own_part, (0, 1, 2)),
        (relay, (0,)),
        (release, (1, 2, 3)),
        (own_part, (3,)),
        (relay, (1,)),
        (choose, (0,)),
        (relay, (2,)),
        (choose, (1,)),
        (relay, (3,)),
        (choose, (2,)),
        (compute, (0,)),
        (choose, (3,)),
        (compute, (1,)),
        (spread_mirrored, (0,)),
        (compute, (2,)),
        (spread_mirrored, (1,)),
        (compute, (3,)),
        (reflect, (0,)),
        (spread_mirrored, (2,)),
        (spread_own, (0,)),
        (reflect, (1,)),
        (spread_mirrored, (3,)),
        (spread_own, (1,)),
        (reflect, (2,)),
        (spread_own, (2, 3)),
        (reflect, (3,)),
        (settle, (0, 1, 2, 3)),
    ):
        for c in chunks:
            stage(c)
    for copy in started:
        copy.wait_send()


def write_out(*refs):
    sources, results, sem = refs[:4], refs[4:8], refs[8]
    copies = [
        pltpu.make_async_copy(src, dst, sem.at[i])
        for i, (src, dst) in enumerate(zip(sources, results, strict=True))
    ]
    for copy in copies:
        copy.start()
    for copy in copies:
        copy.wait()


def on_device(queries, key_states, value_states, grads_out, doc_lengths, block_plan, needed):
    n = lax.axis_size("ctx")
    rows, width = queries.shape
    kv_width = key_states.shape[1]
    own_blocks = rows // BLK
    blocked = (own_blocks, BLK, kv_width)
    listed = needed.shape[1]
    lanes = lane_count(n)
    half = n // lanes // 2
    group_rows = HEADS * rows
    vmem = pl.BlockSpec(memory_space=pltpu.VMEM)
    hbm = pl.BlockSpec(memory_space=pltpu.HBM)
    anywhere = pl.BlockSpec(memory_space=pl.ANY)
    wide = jax.ShapeDtypeStruct((rows, width), jnp.bfloat16)
    narrow = jax.ShapeDtypeStruct((rows, kv_width), jnp.bfloat16)
    results = (wide, wide, narrow, narrow)

    def store(*lead):
        return [pltpu.VMEM((*lead, BLK, HEAD_DIM), jnp.bfloat16)] * PIECES

    def sems(*shape):
        return [pltpu.SemaphoreType.DMA((PIECES, *shape))] * 2

    peers, others = max(lanes - 1, 1), max(half - 1, 1)
    parts = pl.pallas_call(
        functools.partial(kernel, n),
        out_shape=results,
        in_specs=[hbm] * 7,
        out_specs=(vmem,) * 4,
        scratch_shapes=[pltpu.VMEM((rows, width), jnp.bfloat16)] * 2
        + [pltpu.VMEM((rows, kv_width), jnp.float32)] * 2
        + [pltpu.VMEM((rows + listed * BLK, rows), jnp.float32)]
        + [pltpu.SMEM(x.shape, jnp.int32) for x in (doc_lengths, block_plan, needed.T)]
        + [pltpu.VMEM((rows, group_rows), jnp.float32)] * 2
        + [pltpu.VMEM((HEAD_DIM, group_rows), jnp.float32)]
        + [pltpu.VMEM((3, group_rows), jnp.float32)]
        + [pltpu.VMEM((GROUP // PAIR, listed * BLK, PAIR * rows), jnp.float32)] * 2
        + [pltpu.VMEM((GROUP // PAIR, rows + listed * BLK, PAIR * rows), jnp.bfloat16)] * 2
        + store(lanes * 2 * own_blocks)
        + store(others, listed)
        + store(half, listed)
        + store(half, listed)
        + store(peers, 2, own_blocks)
        + store(peers, 2, own_blocks)
        + store(own_blocks)
        + store(own_blocks)
        + [pltpu.SemaphoreType.DMA((2, KV_HEADS))]
        + [pltpu.SemaphoreType.DMA((PIECES,))]
        + [pltpu.SemaphoreType.DMA((3,))]
        + sems()
        + sems(peers)
        + sems(peers)
        + sems(others)
        + sems(others)
        + sems(2, peers)
        + sems(),
        compiler_params=pltpu.CompilerParams(
            collective_id=0, has_side_effects=True, vmem_limit_bytes=48 * 1024 * 1024
        ),
    )(
        *(
            pltpu.with_memory_space_constraint(x, pltpu.HBM)
            for x in (
                queries,
                key_states.reshape(blocked),
                value_states.reshape(blocked),
                grads_out,
                doc_lengths,
                block_plan,
                needed.T,
            )
        )
    )
    return pl.pallas_call(
        write_out,
        out_shape=results,
        in_specs=[vmem] * 4,
        out_specs=(anywhere,) * 4,
        scratch_shapes=[pltpu.SemaphoreType.DMA((4,))],
    )(*(pltpu.with_memory_space_constraint(x, pltpu.VMEM) for x in parts))


def solution(mesh):
    tokens = P(("grp", "ctx"), None)
    return jax.shard_map(
        on_device,
        mesh=mesh,
        in_specs=(tokens, tokens, tokens, tokens, P("grp"), P("grp"), P("grp", None)),
        out_specs=(tokens, tokens, tokens, tokens),
        check_vma=False,
    )
```
